32 devices in a mesh: cuts: 8 (over z, y), event: 4 (over x, core).
Axes of the slice: x: 2, y: 2, z: 4, core: 2. Of those that a mesh axis runs over, the one named last changes fastest.
Arguments:
- kernels: float32 [4, 64, 128, 256], P('event', 'cuts'), may hold values from -24 to 24
- steps: float32 [8, 64, 128, 256], P(None, 'cuts', 'event'), may hold values from -11 to 11
- curvature: float32 [8, 64, 128, 256], P(None, 'cuts', 'event'), may hold values from 0.2 to 5
Outputs:
- gradient: float32 [64, 128, 256], P('cuts', 'event')
- direction: float32 [64, 128, 256], P('cuts', 'event')
The draws below stay inside these ranges and needn't reach their ends.
All inputs are finite; a program needn't handle non-finite values.
Results may differ from the reference program's by a relative error of at most 0.00021.
Values sent between devices are 32-bit elements; how exact they have to be, the bound alone decides.
A program may use at most 64 MiB of HBM per device.

```python
import math
import jax
import jax.numpy as jnp
from jax import lax

NR = 128
NB = 256
PAIRS = 8
RIM = 4
NA = 64
GROUPS = 4


def band_matrix(length, sigma):
    points = jnp.arange(length, dtype=jnp.float32)
    offset = points[:, None] - points[None, :]
    return jnp.exp(-offset * offset / (2.0 * sigma * sigma))


def circle_matrix(length, sigma):
    points = jnp.arange(length, dtype=jnp.float32)
    offset = jnp.abs(points[:, None] - points[None, :])
    offset = jnp.minimum(offset, length - offset)
    return jnp.exp(-offset * offset / (2.0 * sigma * sigma))


def shared_field(key):
    white = jax.random.truncated_normal(jax.random.fold_in(key, 101), -4.0, 4.0, (NA, NR, NB), jnp.float32)
    lon_mat = circle_matrix(NA, 3.0)
    rad_mat = band_matrix(NR, max(2.0, NR / 16.0))
    lat_mat = band_matrix(NB, max(2.0, NB / 32.0))
    field = jnp.einsum('ia,ajb->ijb', lon_mat, white, precision=lax.Precision.HIGHEST)
    field = jnp.einsum('rj,ajb->arb', rad_mat, field, precision=lax.Precision.HIGHEST)
    field = jnp.einsum('ajb,cb->ajc', field, lat_mat, precision=lax.Precision.HIGHEST)
    field = field / jnp.sqrt(jnp.mean(field * field))
    field = jnp.clip(field, -4.0, 4.0)
    return field


def draw_kernels(key, part):
    field = shared_field(key)
    gains = jax.random.uniform(jax.random.fold_in(key, 202), (GROUPS,), jnp.float32, 0.5, 1.5)
    noise = 4.0 * jax.random.truncated_normal(jax.random.fold_in(key, 203), -4.0, 4.0, (GROUPS, NA, NR, NB), jnp.float32)
    return gains[:, None, None, None] * field[None] + noise


def draw_steps(key, part):
    field = shared_field(key)
    factors = jax.random.uniform(jax.random.fold_in(key, 303), (PAIRS,), jnp.float32, 0.3, 1.5)
    noise = jax.random.truncated_normal(jax.random.fold_in(key, 304), -4.0, 4.0, (PAIRS, NA, NR, NB), jnp.float32)
    return -factors[:, None, None, None] * field[None] + noise


def levels(rng, dims, split, smallest, top_value):
    factor_of, own = 1.0, jax.random.fold_in(rng, 6)
    for dim, parts in split:
        steps = jnp.exp(jax.random.uniform(jax.random.fold_in(own, dim), (parts,), jnp.float32, smallest / len(split), top_value / len(split)))
        factor_of = factor_of * jnp.repeat(steps, dims[dim] // parts).reshape([-1 if axis == dim else 1 for axis in range(len(dims))])
    return factor_of


def setup_inputs(seed: int = 0) -> dict:
    streams_of = jax.random.split(jax.random.key(seed), 4)
    kernels = draw_kernels(jax.random.fold_in(streams_of[3], 71), 0)
    steps = draw_steps(jax.random.fold_in(streams_of[3], 71), 0)
    curvature = jnp.clip(jnp.exp(math.log(5.0) - 3.218876 * jax.random.uniform(streams_of[2], (PAIRS, NA, NR, NB), jnp.float32) ** levels(streams_of[2], (PAIRS, NA, NR, NB), ((1, 8), (2, 4)), -0.2, 0.2)), 0.2, 5.0)
    return {"kernels": kernels, "steps": steps, "curvature": curvature}


def gauss_matrix(length, sigma):
    points = jnp.arange(length, dtype=jnp.float32)
    offset = points[:, None] - points[None, :]
    matrix = jnp.exp(-offset * offset / (2.0 * sigma * sigma))
    return matrix / jnp.sum(matrix, axis=1, keepdims=True)


def cycle_weights():
    unscaled = [math.exp(-((column - RIM) ** 2) / 4.5) for column in range(2 * RIM + 1)]
    whole = sum(unscaled)
    return [weight / whole for weight in unscaled]


def reference(kernels, steps, curvature):
    summed = jnp.sum(kernels, axis=0)
    radial = jnp.einsum("ij,ajb->aib", gauss_matrix(summed.shape[1], 3.0), summed, precision=lax.Precision.HIGHEST)
    lat_len = radial.shape[2]
    plane = jnp.dot(radial.reshape(-1, lat_len), gauss_matrix(lat_len, 4.0).T, precision=lax.Precision.HIGHEST).reshape(radial.shape)
    weights = cycle_weights()
    gradient = jnp.zeros_like(plane)
    for column in range(2 * RIM + 1):
        gradient = gradient + weights[column] * jnp.roll(plane, RIM - column, axis=0)
    changes = curvature * steps
    curvs = jnp.sum(changes * steps, axis=(1, 2, 3))
    inverse = 1.0 / curvs
    scaling = curvs[PAIRS - 1] / jnp.sum(changes[PAIRS - 1] * changes[PAIRS - 1])
    carried = gradient
    alphas = [None] * PAIRS
    for pair in reversed(range(PAIRS)):
        alphas[pair] = inverse[pair] * jnp.sum(steps[pair] * carried)
        carried = carried - alphas[pair] * changes[pair]
    result = scaling * carried
    for pair in range(PAIRS):
        second = inverse[pair] * jnp.sum(changes[pair] * result)
        result = result + (alphas[pair] - second) * steps[pair]
    return gradient, -result
```

```python
import functools
import math

import jax
import jax.numpy as jnp
from jax import lax
from jax.experimental import pallas as pl
from jax.experimental.pallas import tpu as pltpu
from jax.sharding import PartitionSpec as P

RIM = 4
LANES = 128
SUB = 8
MESH = pl.DeviceIdType.MESH
HIGHEST = lax.Precision.HIGHEST


def cycle_weights():
    unscaled = [math.exp(-((column - RIM) ** 2) / 4.5) for column in range(2 * RIM + 1)]
    whole = sum(unscaled)
    return [weight / whole for weight in unscaled]


def halves(value):
    high = value.astype(jnp.bfloat16)
    return high, (value - high.astype(jnp.float32)).astype(jnp.bfloat16)


def unscaled_gauss(length, sigma):
    rows = lax.broadcasted_iota(jnp.int32, (length, length), 0)
    columns = lax.broadcasted_iota(jnp.int32, (length, length), 1)
    offset = (rows - columns).astype(jnp.float32)
    return jnp.exp(-offset * offset / (2.0 * sigma * sigma))


def upper(pairs):
    return [(i, j) for i in range(pairs) for j in range(i, pairs)]


def kernel(
    sizes,
    kern_hbm, steps_hbm, curv_hbm, grad_hbm, dir_hbm,
    kern, steps, changes, rad, far_in, near_in, far_out, x_in, plane, lead_in, trail_in,
    grad, direc, rad_mat, lat_mat, gram_acc, gram_tile, gram_event, gram_part, gram_cuts,
    table, splat, mix, coef, late_tile, late_event, late_part, late_cuts,
    load_sem, out_sem, core_send, core_recv, x_send, x_recv, halo_send, halo_recv,
    ge_send, ge_recv, gc_send, gc_recv, le_send, le_recv, lc_send, lc_recv,
):
    n_c, n_e, pairs, rad_len, lat_len = sizes
    part = rad_len // n_e
    c = lax.axis_index("cuts")
    e = lax.axis_index("event")
    barrier = pltpu.get_barrier_semaphore()
    for d in range(1, n_e):
        pl.semaphore_signal(barrier, 1, device_id={"event": lax.rem(e + d, n_e)}, device_id_type=MESH)
    for d in range(1, n_c):
        pl.semaphore_signal(barrier, 1, device_id={"cuts": lax.rem(c + d, n_c)}, device_id_type=MESH)

    loads = [
        pltpu.make_async_copy(kern_hbm.at[:, k], kern.at[:, k], load_sem.at[k]) for k in range(RIM)
    ]
    loads.append(pltpu.make_async_copy(steps_hbm, steps, load_sem.at[RIM]))
    loads.append(pltpu.make_async_copy(curv_hbm, changes, load_sem.at[RIM + 1]))
    for load in loads:
        load.start()

    matrix = unscaled_gauss(rad_len, 3.0)
    high, low = halves(matrix / jnp.sum(matrix, axis=1, keepdims=True))
    rad_mat[...] = jnp.concatenate([high, high, low], axis=1)
    matrix = unscaled_gauss(lat_len, 4.0)
    high, low = halves(matrix / jnp.sum(matrix, axis=0, keepdims=True))
    lat_mat[...] = jnp.concatenate([high, high, low], axis=0)
    gram_tile[...] = jnp.zeros_like(gram_tile)
    late_tile[...] = jnp.zeros_like(late_tile)
    table[...] = jnp.zeros_like(table)

    core = e + 1 - 2 * lax.rem(e, 2)
    far = lax.rem(e + 2, n_e)
    core_far = lax.rem(core + 2, n_e)

    def rows(chunk):
        return pl.ds(pl.multiple_of(chunk * part, part), part)

    def send(src, dst, send_sem, recv_sem, where):
        return pltpu.make_async_remote_copy(
            src_ref=src, dst_ref=dst, send_sem=send_sem, recv_sem=recv_sem,
            device_id=where, device_id_type=MESH,
        )

    far_copies, near_copies, x_copies, halo_copies = [], [], [], []
    for k in range(RIM):
        loads[k].wait()
        for side in range(2):
            high, low = halves(kern[side, k])
            rad[side, k] = jnp.dot(
                rad_mat[...], jnp.concatenate([high, low, high], axis=0),
                preferred_element_type=jnp.float32,
            )
        if k == 0:
            pl.semaphore_wait(barrier, n_e - 1 + n_c - 1)
        far_copies.append(send(
            rad.at[:, k, rows(core_far)], far_in.at[:, k], core_send.at[0, k], core_recv.at[0, k],
            {"event": core},
        ))
        far_copies[-1].start()
    for k in range(RIM):
        near_copies.append(send(
            rad.at[:, k, rows(core)], near_in.at[:, k], core_send.at[1, k], core_recv.at[1, k],
            {"event": core},
        ))
        near_copies[-1].start()
    for k in range(RIM):
        far_copies[k].wait_recv()
        far_out[:, k] = rad[:, k, rows(far)] + far_in[:, k]
        x_copies.append(send(
            far_out.at[:, k], x_in.at[:, k], x_send.at[k], x_recv.at[k], {"event": far}
        ))
        x_copies[-1].start()

    slots = {pair: number for number, pair in enumerate(upper(pairs))}
    count = len(slots)
    groups = [(0, 1), (2, 3), tuple(range(4, pairs))]
    all_rows = steps.shape[1]
    tiles = all_rows // SUB
    lats = lat_len // LANES
    strip = tiles // RIM

    def gram(number):
        if number == 0:
            loads[RIM].wait()
            loads[RIM + 1].wait()

        def scale(t, _):
            place = pl.ds(pl.multiple_of(t * SUB, SUB), SUB)
            for i in range(pairs):
                changes[i, place, :] = changes[i, place, :] * steps[i, place, :]
            return 0

        lax.fori_loop(number * strip, (number + 1) * strip, scale, 0, unroll=2)
        for group in groups:
            wanted = [(i, j) for i in group for j in range(i, pairs)]

            def body(t, sums):
                place = pl.ds(pl.multiple_of(t * SUB, SUB), SUB)
                sums = list(sums)
                for lane in range(lats):
                    across = pl.ds(lane * LANES, LANES)
                    change = {j: changes[j, place, across] for j in range(group[0], pairs)}
                    for n, i in enumerate(group):
                        step = steps[i, place, across]
                        for m, (a, b) in enumerate(wanted):
                            if a == i:
                                sums[2 * m] = sums[2 * m] + step * change[b]
                                sums[2 * m + 1] = sums[2 * m + 1] + change[i] * change[b]
                return tuple(sums)

            sums = lax.fori_loop(
                number * strip, (number + 1) * strip, body,
                tuple(jnp.zeros((SUB, LANES), jnp.float32) for _ in range(2 * len(wanted))),
            )
            for m, pair in enumerate(wanted):
                for kind in range(2):
                    place = slots[pair] + kind * count
                    if number == 0:
                        gram_acc[place] = sums[2 * m + kind]
                    else:
                        gram_acc[place] = gram_acc[place] + sums[2 * m + kind]

    def spread(src, slot_refs, sends, recvs, axis, me, size):
        copies = []
        for d in range(1, size):
            copies.append(send(
                src, slot_refs.at[d - 1], sends.at[d - 1], recvs.at[d - 1],
                {axis: lax.rem(me + d, size)},
            ))
            copies[-1].start()
        return copies

    def gathered(own, slot_refs, copies):
        total = own[...]
        for d, copy in enumerate(copies):
            copy.wait_recv()
            total = total + slot_refs[d]
        return total

    left = lax.rem(c + n_c - 1, n_c)
    right = lax.rem(c + 1, n_c)

    def arrive(k):
        near_copies[k].wait_recv()
        base = rad[:, k, rows(e)] + near_in[:, k]
        x_copies[k].wait_recv()
        whole = (base + x_in[:, k]).reshape(2 * part, lat_len)
        high, low = halves(whole)
        plane[:, k] = jnp.dot(
            jnp.concatenate([high, low, high], axis=1), lat_mat[...],
            preferred_element_type=jnp.float32,
        ).reshape(2, part, lat_len)
        halo_copies.append(send(
            plane.at[0, k], trail_in.at[k], halo_send.at[0, k], halo_recv.at[0, k], {"cuts": left}
        ))
        halo_copies.append(send(
            plane.at[1, k], lead_in.at[k], halo_send.at[1, k], halo_recv.at[1, k], {"cuts": right}
        ))
        halo_copies[-2].start()
        halo_copies[-1].start()

    gram(0)
    gram(1)
    arrive(0)
    gram(2)
    arrive(1)
    gram(3)
    ones = jnp.ones((LANES, LANES), jnp.float32)
    table[pl.ds(0, 2 * count), :] = jnp.sum(gram_acc[...], axis=1)
    gram_tile[...] = lax.dot_general(
        ones[:SUB], table[...], (((1,), (1,)), ((), ())), precision=HIGHEST,
        preferred_element_type=jnp.float32,
    )
    ge_copies = spread(gram_tile, gram_event, ge_send, ge_recv, "event", e, n_e)
    arrive(2)
    gram_part[...] = gathered(gram_tile, gram_event, ge_copies)
    gc_copies = spread(gram_part, gram_cuts, gc_send, gc_recv, "cuts", c, n_c)
    arrive(3)
    products = gathered(gram_part, gram_cuts, gc_copies)
    square = (LANES, LANES)
    on_diagonal = lax.broadcasted_iota(jnp.int32, square, 0) == lax.broadcasted_iota(jnp.int32, square, 1)
    splat[...] = jnp.dot(
        jnp.where(on_diagonal, jnp.broadcast_to(products[:1], square), 0.0), ones,
        precision=HIGHEST, preferred_element_type=jnp.float32,
    )

    def cross(i, j):
        place = slots[i, j]
        return splat[place : place + 1, :]

    def squared(i, j):
        place = count + slots[min(i, j), max(i, j)]
        return splat[place : place + 1, :]

    def unit(place):
        return (lax.broadcasted_iota(jnp.int32, (1, LANES), 1) == place).astype(jnp.float32)

    inverse = [1.0 / cross(i, i) for i in range(pairs)]
    scaling = cross(pairs - 1, pairs - 1) / squared(pairs - 1, pairs - 1)
    alphas = [None] * pairs
    for i in reversed(range(pairs)):
        row = unit(i)
        for j in range(pairs - 1, i, -1):
            row = row - cross(i, j) * alphas[j]
        alphas[i] = inverse[i] * row
    onto = []
    for i in range(pairs):
        row = unit(pairs + i)
        for j in range(pairs):
            row = row - squared(i, j) * alphas[j]
        row = scaling * row
        for j in range(i):
            row = row + cross(j, i) * onto[j]
        onto.append(alphas[i] - inverse[i] * row)
    for i in range(pairs):
        mix[i : i + 1, :] = -onto[i]
        mix[pairs + i : pairs + i + 1, :] = scaling * alphas[i]

    for copy in halo_copies:
        copy.wait_recv()
    weights = cycle_weights()
    lons = 2 * RIM
    sums = [jnp.zeros((SUB, LANES), jnp.float32) for _ in range(2 * pairs)]
    per_plane = part // SUB

    def finish(t, sums):
        sums = list(sums)
        place = pl.ds(pl.multiple_of(t * SUB, SUB), SUB)
        for lane in range(lats):
            across = pl.ds(lane * LANES, LANES)
            padded = (
                [lead_in[k, place, across] for k in range(RIM)]
                + [plane[side, k, place, across] for side in range(2) for k in range(RIM)]
                + [trail_in[k, place, across] for k in range(RIM)]
            )
            for a in range(lons):
                value = weights[RIM] * padded[a + RIM]
                for k in range(1, RIM + 1):
                    value = value + weights[RIM + k] * (padded[a + RIM - k] + padded[a + RIM + k])
                spot = pl.ds(pl.multiple_of(a * part + t * SUB, SUB), SUB)
                grad[spot, across] = value
                for i in range(pairs):
                    sums[i] = sums[i] + value * steps[i, spot, across]
                    sums[pairs + i] = sums[pairs + i] + value * changes[i, spot, across]
        return tuple(sums)

    sums = lax.fori_loop(0, per_plane, finish, tuple(sums))
    for i in range(2 * pairs):
        late_tile[i : i + 1, :] = jnp.sum(sums[i], axis=0, keepdims=True)
    le_copies = spread(late_tile, late_event, le_send, le_recv, "event", e, n_e)
    grad_out = pltpu.make_async_copy(grad, grad_hbm, out_sem.at[0])
    grad_out.start()
    late_part[...] = gathered(late_tile, late_event, le_copies)
    lc_copies = spread(late_part, late_cuts, lc_send, lc_recv, "cuts", c, n_c)
    products = gathered(late_part, late_cuts, lc_copies)
    table[pl.ds(0, 2 * pairs), :] = products
    table[pl.ds(2 * pairs, LANES - 2 * pairs), :] = jnp.zeros(
        (LANES - 2 * pairs, LANES), jnp.float32
    )
    mixed = jnp.dot(mix[...], table[...], precision=HIGHEST, preferred_element_type=jnp.float32)
    coef[...] = jnp.broadcast_to(jnp.sum(mixed, axis=1, keepdims=True), coef.shape)
    ratio = jnp.broadcast_to(-scaling, (SUB, LANES))
    factors = [jnp.broadcast_to(coef[i : i + 1, :], (SUB, LANES)) for i in range(2 * pairs)]

    def combine(t, _):
        place = pl.ds(pl.multiple_of(t * SUB, SUB), SUB)
        for lane in range(lats):
            across = pl.ds(lane * LANES, LANES)
            value = ratio * grad[place, across]
            for i in range(pairs):
                value = value + factors[i] * steps[i, place, across]
                value = value + factors[pairs + i] * changes[i, place, across]
            direc[place, across] = value
        return 0

    lax.fori_loop(0, tiles, combine, 0, unroll=4)
    dir_out = pltpu.make_async_copy(direc, dir_hbm, out_sem.at[1])
    dir_out.start()
    for copies in (far_copies, near_copies, x_copies, halo_copies, ge_copies, gc_copies, le_copies, lc_copies):
        for copy in copies:
            copy.wait_send()
    grad_out.wait()
    dir_out.wait()


def shards(kernels, steps, curvature):
    n_c, n_e = lax.axis_size("cuts"), lax.axis_size("event")
    _, lons, rad_len, lat_len = kernels.shape
    pairs = steps.shape[0]
    part = rad_len // n_e
    assert lons == 2 * RIM and n_e == 4
    all_rows = lons * part
    count = pairs * (pairs + 1)
    f32, bf16 = jnp.float32, jnp.bfloat16
    vmem, dma = pltpu.VMEM, pltpu.SemaphoreType.DMA
    half = (RIM, part, lat_len)
    whole = (2,) + half
    any_spec = pl.BlockSpec(memory_space=pl.ANY)
    out = jax.ShapeDtypeStruct((all_rows, lat_len), f32)
    late = (2 * pairs, LANES)
    gradient, direction = pl.pallas_call(
        functools.partial(kernel, (n_c, n_e, pairs, rad_len, lat_len)),
        out_shape=(out, out),
        in_specs=[any_spec] * 3,
        out_specs=(any_spec, any_spec),
        scratch_shapes=[
            vmem((2, RIM, rad_len, lat_len), f32),
            vmem((pairs, all_rows, lat_len), f32),
            vmem((pairs, all_rows, lat_len), f32),
            vmem((2, RIM, rad_len, lat_len), f32),
            vmem(whole, f32),
            vmem(whole, f32),
            vmem(whole, f32),
            vmem(whole, f32),
            vmem(whole, f32),
            vmem(half, f32),
            vmem(half, f32),
            vmem((all_rows, lat_len), f32),
            vmem((all_rows, lat_len), f32),
            vmem((rad_len, 3 * rad_len), bf16),
            vmem((3 * lat_len, lat_len), bf16),
            vmem((count, SUB, LANES), f32),
            vmem((SUB, LANES), f32),
            vmem((n_e - 1, SUB, LANES), f32),
            vmem((SUB, LANES), f32),
            vmem((n_c - 1, SUB, LANES), f32),
            vmem((LANES, LANES), f32),
            vmem((LANES, LANES), f32),
            vmem((2 * pairs, LANES), f32),
            vmem((2 * pairs, LANES), f32),
            vmem(late, f32),
            vmem((n_e - 1,) + late, f32),
            vmem(late, f32),
            vmem((n_c - 1,) + late, f32),
            dma((RIM + 2,)),
            dma((2,)),
            dma((2, RIM)),
            dma((2, RIM)),
            dma((RIM,)),
            dma((RIM,)),
            dma((2, RIM)),
            dma((2, RIM)),
            dma((n_e - 1,)),
            dma((n_e - 1,)),
            dma((n_c - 1,)),
            dma((n_c - 1,)),
            dma((n_e - 1,)),
            dma((n_e - 1,)),
            dma((n_c - 1,)),
            dma((n_c - 1,)),
        ],
        compiler_params=pltpu.CompilerParams(
            collective_id=0, has_side_effects=True, vmem_limit_bytes=32 * 1024 * 1024
        ),
    )(
        kernels.reshape(2, RIM, rad_len, lat_len),
        steps.reshape(pairs, all_rows, lat_len),
        curvature.reshape(pairs, all_rows, lat_len),
    )
    shape = (lons, part, lat_len)
    return gradient.reshape(shape), direction.reshape(shape)


def solution(mesh):
    placed = (
        P("event", "cuts", None, None),
        P(None, "cuts", "event", None),
        P(None, "cuts", "event", None),
    )
    return jax.shard_map(
        shards,
        mesh=mesh,
        in_specs=placed,
        out_specs=(P("cuts", "event", None), P("cuts", "event", None)),
        check_vma=False,
    )
```

```python
import functools
import math

import jax
import jax.numpy as jnp
from jax import lax
from jax.experimental import pallas as pl
from jax.experimental.pallas import tpu as pltpu
from jax.sharding import PartitionSpec as P

RIM = 4
LANES = 128
SUB = 8
MESH = pl.DeviceIdType.MESH
HIGHEST = lax.Precision.HIGHEST


def cycle_weights():
    unscaled = [math.exp(-((column - RIM) ** 2) / 4.5) for column in range(2 * RIM + 1)]
    whole = sum(unscaled)
    return [weight / whole for weight in unscaled]


def halves(value):
    high = value.astype(jnp.bfloat16)
    return high, (value - high.astype(jnp.float32)).astype(jnp.bfloat16)


def unscaled_gauss(length, sigma):
    rows = lax.broadcasted_iota(jnp.int32, (length, length), 0)
    columns = lax.broadcasted_iota(jnp.int32, (length, length), 1)
    offset = (rows - columns).astype(jnp.float32)
    return jnp.exp(-offset * offset / (2.0 * sigma * sigma))


def upper(pairs):
    return [(i, j) for i in range(pairs) for j in range(i, pairs)]


def kernel(
    sizes,
    kern_hbm, steps_hbm, curv_hbm, grad, steps, changes, coef,
    kern, rad, far_in, near_in, far_out, x_in, plane, lead_in, trail_in,
    rad_mat, lat_mat, gram_acc, gram_row, gram_all,
    table, splat, mix, late_row, late_all,
    load_sem, core_send, core_recv, x_send, x_recv, halo_send, halo_recv,
    gram_send, gram_recv, late_send, late_recv,
):
    n_c, n_e, pairs, rad_len, lat_len = sizes
    part = rad_len // n_e
    c = lax.axis_index("cuts")
    e = lax.axis_index("event")
    barrier = pltpu.get_barrier_semaphore()
    others = [
        {"cuts": lax.rem(c + d // n_e, n_c), "event": lax.rem(e + d % n_e, n_e)}
        for d in range(1, n_c * n_e)
    ]
    for other in others:
        pl.semaphore_signal(barrier, 1, device_id=other, device_id_type=MESH)

    loads = [
        pltpu.make_async_copy(kern_hbm.at[:, k], kern.at[:, k], load_sem.at[k]) for k in range(RIM)
    ]
    loads.append(pltpu.make_async_copy(steps_hbm, steps, load_sem.at[RIM]))
    loads.append(pltpu.make_async_copy(curv_hbm, changes, load_sem.at[RIM + 1]))
    for load in loads:
        load.start()

    matrix = unscaled_gauss(rad_len, 3.0)
    high, low = halves(matrix / jnp.sum(matrix, axis=1, keepdims=True))
    rad_mat[...] = jnp.concatenate([high, high, low], axis=1)
    matrix = unscaled_gauss(lat_len, 4.0)
    high, low = halves(matrix / jnp.sum(matrix, axis=0, keepdims=True))
    lat_mat[...] = jnp.concatenate([high, high, low], axis=0)
    table[...] = jnp.zeros_like(table)

    core = e + 1 - 2 * lax.rem(e, 2)
    far = lax.rem(e + 2, n_e)
    core_far = lax.rem(core + 2, n_e)

    def rows(chunk):
        return pl.ds(pl.multiple_of(chunk * part, part), part)

    def send(src, dst, send_sem, recv_sem, where):
        return pltpu.make_async_remote_copy(
            src_ref=src, dst_ref=dst, send_sem=send_sem, recv_sem=recv_sem,
            device_id=where, device_id_type=MESH,
        )

    far_copies, near_copies, x_copies, halo_copies = [], [], [], []
    for k in range(RIM):
        loads[k].wait()
        for side in range(2):
            high, low = halves(kern[side, k])
            rad[side, k] = jnp.dot(
                rad_mat[...], jnp.concatenate([high, low, high], axis=0),
                preferred_element_type=jnp.float32,
            )
        if k == 0:
            pl.semaphore_wait(barrier, len(others))
        far_copies.append(send(
            rad.at[:, k, rows(core_far)], far_in.at[:, k], core_send.at[0, k], core_recv.at[0, k],
            {"event": core},
        ))
        far_copies[-1].start()
    for k in range(RIM):
        near_copies.append(send(
            rad.at[:, k, rows(core)], near_in.at[:, k], core_send.at[1, k], core_recv.at[1, k],
            {"event": core},
        ))
        near_copies[-1].start()
    for k in range(RIM):
        far_copies[k].wait_recv()
        far_out[:, k] = rad[:, k, rows(far)] + far_in[:, k]
        x_copies.append(send(
            far_out.at[:, k], x_in.at[:, k], x_send.at[k], x_recv.at[k], {"event": far}
        ))
        x_copies[-1].start()

    slots = {pair: number for number, pair in enumerate(upper(pairs))}
    count = len(slots)
    groups = [(0, 1), (2, 3), tuple(range(4, pairs))]
    all_rows = steps.shape[1]
    tiles = all_rows // SUB
    lats = lat_len // LANES
    strip = tiles // RIM

    def gram(number):
        if number == 0:
            loads[RIM].wait()
            loads[RIM + 1].wait()

        def scale(t, _):
            place = pl.ds(pl.multiple_of(t * SUB, SUB), SUB)
            for i in range(pairs):
                changes[i, place, :] = changes[i, place, :] * steps[i, place, :]
            return 0

        lax.fori_loop(number * strip, (number + 1) * strip, scale, 0, unroll=2)
        for group in groups:
            wanted = [(i, j) for i in group for j in range(i, pairs)]

            def body(t, sums):
                place = pl.ds(pl.multiple_of(t * SUB, SUB), SUB)
                sums = list(sums)
                for lane in range(lats):
                    across = pl.ds(lane * LANES, LANES)
                    change = {j: changes[j, place, across] for j in range(group[0], pairs)}
                    for n, i in enumerate(group):
                        step = steps[i, place, across]
                        for m, (a, b) in enumerate(wanted):
                            if a == i:
                                sums[2 * m] = sums[2 * m] + step * change[b]
                                sums[2 * m + 1] = sums[2 * m + 1] + change[i] * change[b]
                return tuple(sums)

            sums = lax.fori_loop(
                number * strip, (number + 1) * strip, body,
                tuple(jnp.zeros((SUB, LANES), jnp.float32) for _ in range(2 * len(wanted))),
            )
            for m, pair in enumerate(wanted):
                for kind in range(2):
                    place = slots[pair] + kind * count
                    if number == 0:
                        gram_acc[place] = sums[2 * m + kind]
                    else:
                        gram_acc[place] = gram_acc[place] + sums[2 * m + kind]

    def spread(row, slot_refs, sends, recvs):
        copies = []
        for d, other in enumerate(others):
            copies.append(send(row, slot_refs.at[d], sends.at[d], recvs.at[d], other))
            copies[-1].start()
        return copies

    def gathered(row, slot_refs, copies):
        for copy in copies:
            copy.wait_recv()
        return row[...] + jnp.sum(slot_refs[...], axis=0)

    left = lax.rem(c + n_c - 1, n_c)
    right = lax.rem(c + 1, n_c)

    def arrive(k):
        near_copies[k].wait_recv()
        base = rad[:, k, rows(e)] + near_in[:, k]
        x_copies[k].wait_recv()
        whole = (base + x_in[:, k]).reshape(2 * part, lat_len)
        high, low = halves(whole)
        plane[:, k] = jnp.dot(
            jnp.concatenate([high, low, high], axis=1), lat_mat[...],
            preferred_element_type=jnp.float32,
        ).reshape(2, part, lat_len)
        halo_copies.append(send(
            plane.at[0, k], trail_in.at[k], halo_send.at[0, k], halo_recv.at[0, k], {"cuts": left}
        ))
        halo_copies.append(send(
            plane.at[1, k], lead_in.at[k], halo_send.at[1, k], halo_recv.at[1, k], {"cuts": right}
        ))
        halo_copies[-2].start()
        halo_copies[-1].start()

    for number in range(RIM):
        gram(number)
    ones = jnp.ones((LANES, LANES), jnp.float32)

    def lane_sums(value):
        return lax.dot_general(
            ones[:SUB], value, (((1,), (1,)), ((), ())), precision=HIGHEST,
            preferred_element_type=jnp.float32,
        )[:1]

    table[pl.ds(0, 2 * count), :] = jnp.sum(gram_acc[...], axis=1)
    gram_row[...] = lane_sums(table[...])
    gram_copies = spread(gram_row, gram_all, gram_send, gram_recv)
    for k in range(RIM):
        arrive(k)
    products = gathered(gram_row, gram_all, gram_copies)
    square = (LANES, LANES)
    on_diagonal = lax.broadcasted_iota(jnp.int32, square, 0) == lax.broadcasted_iota(jnp.int32, square, 1)
    splat[...] = jnp.dot(
        jnp.where(on_diagonal, jnp.broadcast_to(products, square), 0.0), ones,
        precision=HIGHEST, preferred_element_type=jnp.float32,
    )

    def cross(i, j):
        place = slots[i, j]
        return splat[place : place + 1, :]

    def squared(i, j):
        place = count + slots[min(i, j), max(i, j)]
        return splat[place : place + 1, :]

    def unit(place):
        return (lax.broadcasted_iota(jnp.int32, (1, LANES), 1) // SUB == place).astype(jnp.float32)

    inverse = [1.0 / cross(i, i) for i in range(pairs)]
    scaling = cross(pairs - 1, pairs - 1) / squared(pairs - 1, pairs - 1)
    alphas = [None] * pairs
    for i in reversed(range(pairs)):
        row = unit(i)
        for j in range(pairs - 1, i, -1):
            row = row - cross(i, j) * alphas[j]
        alphas[i] = inverse[i] * row
    onto = []
    for i in range(pairs):
        row = unit(pairs + i)
        for j in range(pairs):
            row = row - squared(i, j) * alphas[j]
        row = scaling * row
        for j in range(i):
            row = row + cross(j, i) * onto[j]
        onto.append(alphas[i] - inverse[i] * row)
    for i in range(pairs):
        mix[i : i + 1, :] = -onto[i]
        mix[pairs + i : pairs + i + 1, :] = scaling * alphas[i]

    for copy in halo_copies:
        copy.wait_recv()
    weights = cycle_weights()
    lons = 2 * RIM
    sums = [jnp.zeros((SUB, LANES), jnp.float32) for _ in range(2 * pairs)]
    per_plane = part // SUB

    def finish(t, sums):
        sums = list(sums)
        place = pl.ds(pl.multiple_of(t * SUB, SUB), SUB)
        for lane in range(lats):
            across = pl.ds(lane * LANES, LANES)
            padded = (
                [lead_in[k, place, across] for k in range(RIM)]
                + [plane[side, k, place, across] for side in range(2) for k in range(RIM)]
                + [trail_in[k, place, across] for k in range(RIM)]
            )
            for a in range(lons):
                value = weights[RIM] * padded[a + RIM]
                for k in range(1, RIM + 1):
                    value = value + weights[RIM + k] * (padded[a + RIM - k] + padded[a + RIM + k])
                spot = pl.ds(pl.multiple_of(a * part + t * SUB, SUB), SUB)
                grad[spot, across] = value
                for i in range(pairs):
                    sums[i] = sums[i] + value * steps[i, spot, across]
                    sums[pairs + i] = sums[pairs + i] + value * changes[i, spot, across]
        return tuple(sums)

    sums = lax.fori_loop(0, per_plane, finish, tuple(sums))
    for i in range(2 * pairs):
        table[i * SUB : (i + 1) * SUB, :] = sums[i]
    late_row[...] = lane_sums(table[...])
    late_copies = spread(late_row, late_all, late_send, late_recv)
    products = gathered(late_row, late_all, late_copies)
    mixed = jnp.sum(mix[...] * products, axis=1, keepdims=True)
    coef[pl.ds(0, 2 * pairs), :] = jnp.broadcast_to(mixed, (2 * pairs, LANES))
    coef[pl.ds(2 * pairs, SUB), :] = jnp.broadcast_to(-scaling, (SUB, LANES))
    for copies in (far_copies, near_copies, x_copies, halo_copies, gram_copies, late_copies):
        for copy in copies:
            copy.wait_send()


def combine_kernel(pairs, blocks, grad, steps, changes, coef, grad_hbm, dir_hbm, direc, sems):
    grad_out = pltpu.make_async_copy(grad, grad_hbm, sems.at[blocks])
    grad_out.start()
    all_rows, lat_len = grad.shape
    ratio = jnp.broadcast_to(coef[2 * pairs : 2 * pairs + 1, :], (SUB, LANES))
    factors = [jnp.broadcast_to(coef[i : i + 1, :], (SUB, LANES)) for i in range(2 * pairs)]
    tiles = all_rows // SUB // blocks

    def combine(t, _):
        place = pl.ds(pl.multiple_of(t * SUB, SUB), SUB)
        for lane in range(lat_len // LANES):
            across = pl.ds(lane * LANES, LANES)
            value = ratio * grad[place, across]
            for i in range(pairs):
                value = value + factors[i] * steps[i, place, across]
                value = value + factors[pairs + i] * changes[i, place, across]
            direc[place, across] = value
        return 0

    copies = []
    for block in range(blocks):
        lax.fori_loop(block * tiles, (block + 1) * tiles, combine, 0, unroll=4)
        place = pl.ds(block * tiles * SUB, tiles * SUB)
        copies.append(pltpu.make_async_copy(direc.at[place], dir_hbm.at[place], sems.at[block]))
        copies[-1].start()
    grad_out.wait()
    for copy in copies:
        copy.wait()


def shards(kernels, steps, curvature):
    n_c, n_e = lax.axis_size("cuts"), lax.axis_size("event")
    _, lons, rad_len, lat_len = kernels.shape
    pairs = steps.shape[0]
    part = rad_len // n_e
    assert lons == 2 * RIM and n_e == 4
    all_rows = lons * part
    count = pairs * (pairs + 1)
    f32, bf16 = jnp.float32, jnp.bfloat16
    vmem, dma = pltpu.VMEM, pltpu.SemaphoreType.DMA
    half = (RIM, part, lat_len)
    whole = (2,) + half
    vmem_spec = pl.BlockSpec(memory_space=pltpu.VMEM)
    any_spec = pl.BlockSpec(memory_space=pl.ANY)
    out = jax.ShapeDtypeStruct((all_rows, lat_len), f32)
    others = n_c * n_e - 1
    assert 2 * pairs * SUB == LANES
    staged = pl.pallas_call(
        functools.partial(kernel, (n_c, n_e, pairs, rad_len, lat_len)),
        out_shape=(
            vmem((all_rows, lat_len), f32),
            vmem((pairs, all_rows, lat_len), f32),
            vmem((pairs, all_rows, lat_len), f32),
            vmem((2 * pairs + SUB, LANES), f32),
        ),
        in_specs=[any_spec] * 3,
        out_specs=(vmem_spec,) * 4,
        scratch_shapes=[
            vmem((2, RIM, rad_len, lat_len), f32),
            vmem((2, RIM, rad_len, lat_len), f32),
            vmem(whole, f32),
            vmem(whole, f32),
            vmem(whole, f32),
            vmem(whole, f32),
            vmem(whole, f32),
            vmem(half, f32),
            vmem(half, f32),
            vmem((rad_len, 3 * rad_len), bf16),
            vmem((3 * lat_len, lat_len), bf16),
            vmem((count, SUB, LANES), f32),
            vmem((1, LANES), f32),
            vmem((others, 1, LANES), f32),
            vmem((LANES, LANES), f32),
            vmem((LANES, LANES), f32),
            vmem((2 * pairs, LANES), f32),
            vmem((1, LANES), f32),
            vmem((others, 1, LANES), f32),
            dma((RIM + 2,)),
            dma((2, RIM)),
            dma((2, RIM)),
            dma((RIM,)),
            dma((RIM,)),
            dma((2, RIM)),
            dma((2, RIM)),
            dma((others,)),
            dma((others,)),
            dma((others,)),
            dma((others,)),
        ],
        compiler_params=pltpu.CompilerParams(
            collective_id=0, has_side_effects=True, vmem_limit_bytes=61905306
        ),
    )(
        kernels.reshape(2, RIM, rad_len, lat_len),
        steps.reshape(pairs, all_rows, lat_len),
        curvature.reshape(pairs, all_rows, lat_len),
    )
    blocks = 4
    gradient, direction = pl.pallas_call(
        functools.partial(combine_kernel, pairs, blocks),
        out_shape=(out, out),
        in_specs=[vmem_spec] * 4,
        out_specs=(any_spec, any_spec),
        scratch_shapes=[vmem((all_rows, lat_len), f32), dma((blocks + 1,))],
        compiler_params=pltpu.CompilerParams(vmem_limit_bytes=2 * 1024 * 1024),
    )(*staged)
    shape = (lons, part, lat_len)
    return gradient.reshape(shape), direction.reshape(shape)


def solution(mesh):
    placed = (
        P("event", "cuts", None, None),
        P(None, "cuts", "event", None),
        P(None, "cuts", "event", None),
    )
    return jax.shard_map(
        shards,
        mesh=mesh,
        in_specs=placed,
        out_specs=(P("cuts", "event", None), P("cuts", "event", None)),
        check_vma=False,
    )
```

```python
import functools
import math

import jax
import jax.numpy as jnp
from jax import lax
from jax.experimental import pallas as pl
from jax.experimental.pallas import tpu as pltpu
from jax.sharding import PartitionSpec as P

RIM = 4
SPLIT = 2
LANES = 128
SUB = 8
MESH = pl.DeviceIdType.MESH
HIGHEST = lax.Precision.HIGHEST


def cycle_weights():
    unscaled = [math.exp(-((column - RIM) ** 2) / 4.5) for column in range(2 * RIM + 1)]
    whole = sum(unscaled)
    return [weight / whole for weight in unscaled]


def halves(value):
    high = value.astype(jnp.bfloat16)
    return high, (value - high.astype(jnp.float32)).astype(jnp.bfloat16)


def unscaled_gauss(length, sigma):
    rows = lax.broadcasted_iota(jnp.int32, (length, length), 0)
    columns = lax.broadcasted_iota(jnp.int32, (length, length), 1)
    offset = (rows - columns).astype(jnp.float32)
    return jnp.exp(-offset * offset / (2.0 * sigma * sigma))


def upper(pairs):
    return [(i, j) for i in range(pairs) for j in range(i, pairs)]


def kernel(
    sizes,
    kern_hbm, steps_hbm, curv_hbm, grad, steps, changes, coef,
    kern, rad, far_in, near_in, far_out, x_in, plane, halo_in,
    rad_mat, lat_mat, gram_acc, gram_row, gram_all,
    table, splat, mix, late_row, late_all,
    load_sem, core_send, core_recv, x_send, x_recv, halo_send, halo_recv,
    gram_send, gram_recv, late_send, late_recv,
):
    n_c, n_e, pairs, rad_len, lat_len = sizes
    part = rad_len // n_e
    c = lax.axis_index("cuts")
    e = lax.axis_index("event")
    barrier = pltpu.get_barrier_semaphore()
    others = [
        {"cuts": lax.rem(c + d // n_e, n_c), "event": lax.rem(e + d % n_e, n_e)}
        for d in range(1, n_c * n_e)
    ]
    for other in others:
        pl.semaphore_signal(barrier, 1, device_id=other, device_id_type=MESH)

    loads = [
        pltpu.make_async_copy(kern_hbm.at[:, k], kern.at[:, k], load_sem.at[k]) for k in range(RIM)
    ]
    loads.append(pltpu.make_async_copy(steps_hbm, steps, load_sem.at[RIM]))
    loads.append(pltpu.make_async_copy(curv_hbm, changes, load_sem.at[RIM + 1]))
    for load in loads:
        load.start()

    matrix = unscaled_gauss(rad_len, 3.0)
    high, low = halves(matrix / jnp.sum(matrix, axis=1, keepdims=True))
    rad_mat[...] = jnp.concatenate([high, high, low], axis=1)
    matrix = unscaled_gauss(lat_len, 4.0)
    high, low = halves(matrix / jnp.sum(matrix, axis=0, keepdims=True))
    lat_mat[...] = jnp.concatenate([high, high, low], axis=0)
    table[...] = jnp.zeros_like(table)

    core = e + 1 - 2 * lax.rem(e, 2)
    far = lax.rem(e + 2, n_e)
    core_far = lax.rem(core + 2, n_e)

    def rows(chunk):
        return pl.ds(pl.multiple_of(chunk * part, part), part)

    def send(src, dst, send_sem, recv_sem, where):
        return pltpu.make_async_remote_copy(
            src_ref=src, dst_ref=dst, send_sem=send_sem, recv_sem=recv_sem,
            device_id=where, device_id_type=MESH,
        )

    far_copies, near_copies, x_copies, halo_copies = [], [], [], []
    for k in range(RIM):
        loads[k].wait()
        for side in range(2):
            high, low = halves(kern[side, k])
            rad[side, k] = jnp.dot(
                rad_mat[...], jnp.concatenate([high, low, high], axis=0),
                preferred_element_type=jnp.float32,
            )
    pl.semaphore_wait(barrier, len(others))
    for k in range(RIM):
        far_copies.append(send(
            rad.at[:, k, rows(core_far)], far_in.at[:, k], core_send.at[0, k], core_recv.at[0, k],
            {"event": core},
        ))
        far_copies[-1].start()
    for k in range(RIM):
        near_copies.append(send(
            rad.at[:, k, rows(core)], near_in.at[:, k], core_send.at[1, k], core_recv.at[1, k],
            {"event": core},
        ))
        near_copies[-1].start()
    strips = part // SUB
    step_k = RIM // SPLIT
    pieces = [(h, g) for h in range(strips) for g in range(SPLIT)]

    def strip_rows(chunk, h):
        return pl.ds(pl.multiple_of(chunk * part + h * SUB, SUB), SUB)

    for h, g in pieces:
        ks = pl.ds(g * step_k, step_k)
        if h == 0:
            for k in range(g * step_k, (g + 1) * step_k):
                far_copies[k].wait_recv()
        here = pl.ds(h * SUB, SUB)
        far_out[:, ks, here] = rad[:, ks, strip_rows(far, h)] + far_in[:, ks, here]
        x_copies.append(send(
            far_out.at[:, ks, here], x_in.at[:, ks, here], x_send.at[h, g], x_recv.at[h, g],
            {"event": far},
        ))
        x_copies[-1].start()

    slots = {pair: number for number, pair in enumerate(upper(pairs))}
    count = len(slots)
    groups = [(0, 1), (2, 3), tuple(range(4, pairs))]
    all_rows = steps.shape[1]
    tiles = all_rows // SUB
    lats = lat_len // LANES
    strip = tiles // RIM

    def gram(number):
        if number == 0:
            loads[RIM].wait()
            loads[RIM + 1].wait()

        def scale(t, _):
            place = pl.ds(pl.multiple_of(t * SUB, SUB), SUB)
            for i in range(pairs):
                changes[i, place, :] = changes[i, place, :] * steps[i, place, :]
            return 0

        lax.fori_loop(number * strip, (number + 1) * strip, scale, 0, unroll=2)
        for group in groups:
            wanted = [(i, j) for i in group for j in range(i, pairs)]

            def body(t, sums):
                place = pl.ds(pl.multiple_of(t * SUB, SUB), SUB)
                sums = list(sums)
                for lane in range(lats):
                    across = pl.ds(lane * LANES, LANES)
                    change = {j: changes[j, place, across] for j in range(group[0], pairs)}
                    for n, i in enumerate(group):
                        step = steps[i, place, across]
                        for m, (a, b) in enumerate(wanted):
                            if a == i:
                                sums[2 * m] = sums[2 * m] + step * change[b]
                                sums[2 * m + 1] = sums[2 * m + 1] + change[i] * change[b]
                return tuple(sums)

            sums = lax.fori_loop(
                number * strip, (number + 1) * strip, body,
                tuple(jnp.zeros((SUB, LANES), jnp.float32) for _ in range(2 * len(wanted))),
            )
            for m, pair in enumerate(wanted):
                for kind in range(2):
                    place = slots[pair] + kind * count
                    if number == 0:
                        gram_acc[place] = sums[2 * m + kind]
                    else:
                        gram_acc[place] = gram_acc[place] + sums[2 * m + kind]

    def spread(row, slot_refs, sends, recvs):
        copies = []
        for d, other in enumerate(others):
            copies.append(send(row, slot_refs.at[d], sends.at[d], recvs.at[d], other))
            copies[-1].start()
        return copies

    def gathered(row, slot_refs, copies):
        for copy in copies:
            copy.wait_recv()
        return row[...] + jnp.sum(slot_refs[...], axis=0)

    def arrive(h):
        here = pl.ds(h * SUB, SUB)
        for g in range(SPLIT):
            ks = pl.ds(g * step_k, step_k)
            if h == 0:
                for k in range(g * step_k, (g + 1) * step_k):
                    near_copies[k].wait_recv()
            base = rad[:, ks, strip_rows(e, h)] + near_in[:, ks, here]
            x_copies[h * SPLIT + g].wait_recv()
            whole = (base + x_in[:, ks, here]).reshape(2 * step_k * SUB, lat_len)
            high, low = halves(whole)
            plane[:, ks, here] = jnp.dot(
                jnp.concatenate([high, low, high], axis=1), lat_mat[...],
                preferred_element_type=jnp.float32,
            ).reshape(2, step_k, SUB, lat_len)
            odd = lax.rem(c, 2)
            for side in (odd, 1 - odd):
                halo_copies.append(send(
                    plane.at[side, ks, here], halo_in.at[side, ks, here],
                    halo_send.at[side, h, g], halo_recv.at[side, h, g],
                    {"cuts": lax.rem(c + n_c - 1 + 2 * side, n_c)},
                ))
                halo_copies[-1].start()

    weights = cycle_weights()
    lons = 2 * RIM

    def finish(h):
        for copy in halo_copies[2 * SPLIT * h : 2 * SPLIT * (h + 1)]:
            copy.wait_recv()
        sums = [None] * (2 * pairs)
        for lane in range(lats):
            place, across = pl.ds(h * SUB, SUB), pl.ds(lane * LANES, LANES)
            padded = (
                [halo_in[1, k, place, across] for k in range(RIM)]
                + [plane[side, k, place, across] for side in range(2) for k in range(RIM)]
                + [halo_in[0, k, place, across] for k in range(RIM)]
            )
            for a in range(lons):
                value = weights[RIM] * padded[a + RIM]
                for k in range(1, RIM + 1):
                    value = value + weights[RIM + k] * (padded[a + RIM - k] + padded[a + RIM + k])
                spot = pl.ds(a * part + h * SUB, SUB)
                grad[spot, across] = value
                for i in range(pairs):
                    for n, vector in ((i, steps), (pairs + i, changes)):
                        term = value * vector[i, spot, across]
                        sums[n] = term if sums[n] is None else sums[n] + term
        for n in range(2 * pairs):
            place = pl.ds(n * SUB, SUB)
            table[place, :] = sums[n] if h == 0 else table[place, :] + sums[n]

    gram(0)
    gram(1)
    arrive(0)
    gram(2)
    arrive(1)
    gram(3)
    ones = jnp.ones((LANES, LANES), jnp.float32)

    def lane_sums(value):
        return lax.dot_general(
            ones[:SUB], value, (((1,), (1,)), ((), ())), precision=HIGHEST,
            preferred_element_type=jnp.float32,
        )[:1]

    table[pl.ds(0, 2 * count), :] = jnp.sum(gram_acc[...], axis=1)
    gram_row[...] = lane_sums(table[...])
    gram_copies = spread(gram_row, gram_all, gram_send, gram_recv)
    for h in range(2, strips):
        arrive(h)
    for h in range(strips):
        finish(h)
    first, _ = halves(table[...])
    second, third = halves(table[...] - first.astype(jnp.float32))
    late_row[...] = lax.dot_general(
        jnp.ones((SUB, 3 * LANES), jnp.bfloat16), jnp.concatenate([first, second, third], axis=1),
        (((1,), (1,)), ((), ())), preferred_element_type=jnp.float32,
    )[:1]
    late_copies = spread(late_row, late_all, late_send, late_recv)
    products = gathered(gram_row, gram_all, gram_copies)
    square = (LANES, LANES)
    on_diagonal = lax.broadcasted_iota(jnp.int32, square, 0) == lax.broadcasted_iota(jnp.int32, square, 1)
    splat[...] = jnp.dot(
        jnp.where(on_diagonal, jnp.broadcast_to(products, square), 0.0), ones,
        precision=HIGHEST, preferred_element_type=jnp.float32,
    )

    def cross(i, j):
        place = slots[i, j]
        return splat[place : place + 1, :]

    def squared(i, j):
        place = count + slots[min(i, j), max(i, j)]
        return splat[place : place + 1, :]

    def unit(place):
        return (lax.broadcasted_iota(jnp.int32, (1, LANES), 1) // SUB == place).astype(jnp.float32)

    inverse = [1.0 / cross(i, i) for i in range(pairs)]
    scaling = cross(pairs - 1, pairs - 1) / squared(pairs - 1, pairs - 1)
    alphas = [None] * pairs
    for i in reversed(range(pairs)):
        row = unit(i)
        for j in range(pairs - 1, i, -1):
            row = row - cross(i, j) * alphas[j]
        alphas[i] = inverse[i] * row
    onto = []
    for i in range(pairs):
        row = unit(pairs + i)
        for j in range(pairs):
            row = row - squared(i, j) * alphas[j]
        row = scaling * row
        for j in range(i):
            row = row + cross(j, i) * onto[j]
        onto.append(alphas[i] - inverse[i] * row)
    for i in range(pairs):
        mix[i : i + 1, :] = -onto[i]
        mix[pairs + i : pairs + i + 1, :] = scaling * alphas[i]

    products = gathered(late_row, late_all, late_copies)
    mixed = jnp.sum(mix[...] * products, axis=1, keepdims=True)
    coef[pl.ds(0, 2 * pairs), :] = jnp.broadcast_to(mixed, (2 * pairs, LANES))
    coef[pl.ds(2 * pairs, SUB), :] = jnp.broadcast_to(-scaling, (SUB, LANES))
    for copies in (far_copies, near_copies, x_copies, halo_copies, gram_copies, late_copies):
        for copy in copies:
            copy.wait_send()


def combine_kernel(pairs, blocks, grad, steps, changes, coef, grad_hbm, dir_hbm, direc, sems):
    grad_out = pltpu.make_async_copy(grad, grad_hbm, sems.at[blocks])
    grad_out.start()
    all_rows, lat_len = grad.shape
    ratio = jnp.broadcast_to(coef[2 * pairs : 2 * pairs + 1, :], (SUB, LANES))
    factors = [jnp.broadcast_to(coef[i : i + 1, :], (SUB, LANES)) for i in range(2 * pairs)]
    tiles = all_rows // SUB // blocks

    def combine(t, _):
        place = pl.ds(pl.multiple_of(t * SUB, SUB), SUB)
        for lane in range(lat_len // LANES):
            across = pl.ds(lane * LANES, LANES)
            value = ratio * grad[place, across]
            for i in range(pairs):
                value = value + factors[i] * steps[i, place, across]
                value = value + factors[pairs + i] * changes[i, place, across]
            direc[place, across] = value
        return 0

    copies = []
    for block in range(blocks):
        lax.fori_loop(block * tiles, (block + 1) * tiles, combine, 0, unroll=4)
        place = pl.ds(block * tiles * SUB, tiles * SUB)
        copies.append(pltpu.make_async_copy(direc.at[place], dir_hbm.at[place], sems.at[block]))
        copies[-1].start()
    grad_out.wait()
    for copy in copies:
        copy.wait()


def shards(kernels, steps, curvature):
    n_c, n_e = lax.axis_size("cuts"), lax.axis_size("event")
    _, lons, rad_len, lat_len = kernels.shape
    pairs = steps.shape[0]
    part = rad_len // n_e
    assert lons == 2 * RIM and n_e == 4
    all_rows = lons * part
    count = pairs * (pairs + 1)
    f32, bf16 = jnp.float32, jnp.bfloat16
    vmem, dma = pltpu.VMEM, pltpu.SemaphoreType.DMA
    half = (RIM, part, lat_len)
    whole = (2,) + half
    vmem_spec = pl.BlockSpec(memory_space=pltpu.VMEM)
    any_spec = pl.BlockSpec(memory_space=pl.ANY)
    out = jax.ShapeDtypeStruct((all_rows, lat_len), f32)
    others = n_c * n_e - 1
    assert 2 * pairs * SUB == LANES
    staged = pl.pallas_call(
        functools.partial(kernel, (n_c, n_e, pairs, rad_len, lat_len)),
        out_shape=(
            vmem((all_rows, lat_len), f32),
            vmem((pairs, all_rows, lat_len), f32),
            vmem((pairs, all_rows, lat_len), f32),
            vmem((2 * pairs + SUB, LANES), f32),
        ),
        in_specs=[any_spec] * 3,
        out_specs=(vmem_spec,) * 4,
        scratch_shapes=[
            vmem((2, RIM, rad_len, lat_len), f32),
            vmem((2, RIM, rad_len, lat_len), f32),
            vmem(whole, f32),
            vmem(whole, f32),
            vmem(whole, f32),
            vmem(whole, f32),
            vmem(whole, f32),
            vmem(whole, f32),
            vmem((rad_len, 3 * rad_len), bf16),
            vmem((3 * lat_len, lat_len), bf16),
            vmem((count, SUB, LANES), f32),
            vmem((1, LANES), f32),
            vmem((others, 1, LANES), f32),
            vmem((LANES, LANES), f32),
            vmem((LANES, LANES), f32),
            vmem((2 * pairs, LANES), f32),
            vmem((1, LANES), f32),
            vmem((others, 1, LANES), f32),
            dma((RIM + 2,)),
            dma((2, RIM)),
            dma((2, RIM)),
            dma((part // SUB, SPLIT)),
            dma((part // SUB, SPLIT)),
            dma((2, part // SUB, SPLIT)),
            dma((2, part // SUB, SPLIT)),
            dma((others,)),
            dma((others,)),
            dma((others,)),
            dma((others,)),
        ],
        compiler_params=pltpu.CompilerParams(
            collective_id=0, has_side_effects=True, vmem_limit_bytes=61905306
        ),
    )(
        kernels.reshape(2, RIM, rad_len, lat_len),
        steps.reshape(pairs, all_rows, lat_len),
        curvature.reshape(pairs, all_rows, lat_len),
    )
    blocks = 4
    gradient, direction = pl.pallas_call(
        functools.partial(combine_kernel, pairs, blocks),
        out_shape=(out, out),
        in_specs=[vmem_spec] * 4,
        out_specs=(any_spec, any_spec),
        scratch_shapes=[vmem((all_rows, lat_len), f32), dma((blocks + 1,))],
        compiler_params=pltpu.CompilerParams(vmem_limit_bytes=2 * 1024 * 1024),
    )(*staged)
    shape = (lons, part, lat_len)
    return gradient.reshape(shape), direction.reshape(shape)


def solution(mesh):
    placed = (
        P("event", "cuts", None, None),
        P(None, "cuts", "event", None),
        P(None, "cuts", "event", None),
    )
    return jax.shard_map(
        shards,
        mesh=mesh,
        in_specs=placed,
        out_specs=(P("cuts", "event", None), P("cuts", "event", None)),
        check_vma=False,
    )
```
